32 devices in a mesh: expert: 2 (over y), tensor: 16 (over z, x, core).
Axes of the slice: x: 2, y: 2, z: 4, core: 2. Of those that a mesh axis runs over, the one named last changes fastest.
Arguments:
- tokens: bfloat16 [256, 6144], P(('expert', 'tensor')), may hold values from -6 to 6
- expert_ids: int32 [256, 2], P(('expert', 'tensor')), may hold values from 0 to 7, all different within a row; in each aligned block of 8 rows (0 to 7, 8 to 15, ...) at most 3 rows name the same one
- gates: float32 [256, 2], P(('expert', 'tensor')), may hold values from 0.2 to 1
- w_gate: bfloat16 [8, 6144, 8192], P('expert', None, 'tensor'), may hold values from -0.078125 to 0.078125
- w_up: bfloat16 [8, 6144, 8192], P('expert', None, 'tensor'), may hold values from -0.078125 to 0.078125
- w_down: bfloat16 [8, 8192, 6144], P('expert', 'tensor'), may hold values from -0.0625 to 0.0625
Outputs:
- mixed: bfloat16 [256, 6144], P(('expert', 'tensor'))
The draws below stay inside these ranges and needn't reach their ends.
Inputs may be any that keep to these rules, and one draw needn't show every extreme that they name: `expert_ids`: each token names 2 different experts. Among the tokens of one device (aligned blocks of 8 rows) no expert is named more than 3 times, a bound that some expert reaches in every block.
All inputs are finite; a program needn't handle non-finite values.
Results may differ from the reference program's by a relative error of at most 0.02.
Values may be sent and summed in bfloat16 or wider, within the bound.
A program may use at most 128 MiB of HBM per device.

```python
import math
import jax
import jax.numpy as jnp
import numpy as np
from jax import lax

D = 6144
FF = 8192
EXPERTS = 8
TOPK = 2
TOK_DEV = 8
CAP = 3
TOKENS = 256
N_EXPERT = 2
N_TENSOR = 16


def level_of(key, dims, split, least, top_value):
    def one(axis_at, parts):
        draws = jax.random.uniform(jax.random.fold_in(jax.random.fold_in(key, 6), axis_at), (parts,), jnp.float32, least / len(split), top_value / len(split))
        return jnp.repeat(jnp.exp(draws), dims[axis_at] // parts).reshape((-1,) + (1,) * (len(dims) - axis_at - 1))

    gain = one(*split[0])
    for cut in split[1:]:
        gain = gain * one(*cut)
    return gain


def routed_block(own_key, own, number, rows, count, top, bound, skew):
    order = jax.random.permutation(own_key, count)
    heavy_load, usual = shares(count, rows * top, bound, skew, True), shares(count, rows * top, bound, skew, False)
    places = jnp.arange(count)

    def named(lengths, turn):
        used = int((lengths > 0).sum())
        fixed = max(1, used // 4)
        shifted = fixed + (places - fixed + turn * (used - fixed)) % max(1, count - fixed)
        return jnp.zeros((count,), jnp.int32).at[order[jnp.where(places < fixed, places, shifted)]].set(jnp.asarray(lengths, jnp.int32))

    lengths = jnp.where(number % 4 == 0, named(heavy_load, number // 4), named(usual, number - number // 4 - 1))
    mixed = jax.random.permutation(jax.random.fold_in(own, 3), count)
    giver, sink = mixed[0:count // 2 * 2:2], mixed[1:count // 2 * 2:2]
    room = jnp.minimum(lengths[giver] - 1, bound - lengths[sink]) // 2
    room = jnp.where((giver == order[0]) | (sink == order[0]) | (lengths[sink] == 0), 0, jnp.maximum(room, 0))
    shifted = jax.random.randint(jax.random.fold_in(own, 4), (count // 2,), 0, 1 << 20) % (room + 1)
    lengths = lengths.at[giver].add(-shifted).at[sink].add(shifted)
    labels = jnp.searchsorted(jnp.cumsum(lengths), jnp.arange(rows * top), side="right").astype(jnp.int32)
    table = labels.reshape(top, rows).T
    table = table[jax.random.permutation(jax.random.fold_in(own, 1), rows)]
    turn = jax.random.randint(jax.random.fold_in(own, 2), (rows, 1), 0, top)
    return jnp.take_along_axis(table, (jnp.arange(top)[None, :] + turn) % top, axis=1)


def shares(count, total, most, skew, full):
    portions = [(1 << 20) // math.isqrt(grade ** skew) + 1 for grade in range(1, count + 1)]
    largest = most if full else min(most, max(-(-total // count), total * portions[0] // sum(portions)))
    least = 1 if total - largest >= count - 1 else 0
    counts, rest = [largest] + [least] * (count - 1), total - largest - least * (count - 1)
    while rest > 0:
        free = [i for i in range(1, count) if counts[i] < largest] or [i for i in range(1, count) if counts[i] < most]
        pool, budget = sum([portions[i] for i in free]), rest
        for i in free:
            addition = min(most - counts[i], max(1, budget * portions[i] // pool), rest)
            counts[i] = counts[i] + addition
            rest = rest - addition
    return np.array(counts)


def scatter_about(rng, shape, scale, bound, cuts=(), held_as=jnp.bfloat16):
    result = scale * jax.random.normal(rng, shape, jnp.float32)
    if cuts:
        result = result * level_of(rng, shape, cuts, -0.22, 0.18)
    return jnp.clip(result, -bound, bound).astype(held_as)


def setup_inputs(seed: int = 0) -> dict:
    arg_keys = jax.random.split(jax.random.key(seed), 7)
    tokens = scatter_about(arg_keys[0], (TOKENS, D), 1.0, 6.0, ((0, 32),))
    expert_ids_keys = jax.random.split(jax.random.fold_in(arg_keys[1], 1), TOKENS // TOK_DEV)
    expert_ids_turns = jax.random.permutation(jax.random.fold_in(arg_keys[1], 3), TOKENS // TOK_DEV)
    expert_ids = jax.vmap(lambda own, number: routed_block(jax.random.fold_in(arg_keys[1], 2), own, number, TOK_DEV, EXPERTS, TOPK, CAP, 2))(expert_ids_keys, expert_ids_turns).reshape((TOKENS, TOPK))
    gates = jnp.clip(0.2 + 0.8 * jax.random.uniform(arg_keys[2], (TOKENS, TOPK), jnp.float32) ** level_of(arg_keys[2], (TOKENS, TOPK), ((0, 32),), -0.2, 0.2), 0.2, 1.0)
    w_gate = scatter_about(arg_keys[3], (EXPERTS, D, FF), D ** -0.5, 0.078125, ((0, 2), (2, 16)))
    w_up = scatter_about(arg_keys[4], (EXPERTS, D, FF), D ** -0.5, 0.078125, ((0, 2), (2, 16)))
    w_down = scatter_about(arg_keys[5], (EXPERTS, FF, D), FF ** -0.5, 0.0625, ((0, 2), (1, 16)))
    return dict(tokens=tokens, expert_ids=expert_ids, gates=gates, w_gate=w_gate, w_up=w_up, w_down=w_down)


def route_places(ids):
    flat = ids.reshape(-1).astype(jnp.int32)
    onehot = (flat[:, None] == jnp.arange(EXPERTS, dtype=jnp.int32)[None, :]).astype(jnp.int32)
    before = jnp.cumsum(onehot, axis=0) - onehot
    slot = jnp.sum(before * onehot, axis=1)
    return (flat * CAP + slot).astype(jnp.int32)


def dispatch_block(rows, places):
    picker = (jnp.arange(EXPERTS * CAP, dtype=jnp.int32)[:, None] == places[None, :]).astype(jnp.bfloat16)
    doubled = jnp.repeat(rows, TOPK, axis=0)
    return jnp.dot(picker, doubled, preferred_element_type=jnp.float32).astype(jnp.bfloat16)


def combine_block(gate_rows, places, results):
    weights = (jnp.arange(EXPERTS * CAP, dtype=jnp.int32)[None, :] == places[:, None]).astype(jnp.float32)
    weights = weights * gate_rows.reshape(-1)[:, None]
    weights = jnp.sum(weights.reshape(TOK_DEV, TOPK, EXPERTS * CAP), axis=1)
    return jnp.dot(weights, results.astype(jnp.float32), precision=lax.Precision.HIGHEST).astype(jnp.bfloat16)


def expert_ffn(item):
    rows, gate_matrix, up_matrix, down_matrix = item
    shard = FF // N_TENSOR
    gate_act = jnp.dot(rows, gate_matrix, preferred_element_type=jnp.float32)
    up_act = jnp.dot(rows, up_matrix, preferred_element_type=jnp.float32)
    hidden = (jax.nn.silu(gate_act) * up_act).astype(jnp.bfloat16)
    pieces = hidden.reshape(rows.shape[0], N_TENSOR, shard).transpose(1, 0, 2)
    downs = down_matrix.reshape(N_TENSOR, shard, D)

    def add_part(total, pair):
        part = jnp.dot(pair[0], pair[1], preferred_element_type=jnp.float32).astype(jnp.bfloat16)
        part = lax.optimization_barrier(part)
        return total + part.astype(jnp.float32), None

    total, _ = lax.scan(add_part, jnp.zeros((rows.shape[0], D), jnp.float32), (pieces, downs))
    return total.astype(jnp.bfloat16)


def reference(tokens, expert_ids, gates, w_gate, w_up, w_down):
    blocks = N_EXPERT * N_TENSOR
    token_blocks = tokens.reshape(blocks, TOK_DEV, D)
    id_blocks = expert_ids.reshape(blocks, TOK_DEV, TOPK)
    gate_blocks = gates.reshape(blocks, TOK_DEV, TOPK)
    places = jax.vmap(route_places)(id_blocks)
    buffers = jax.vmap(dispatch_block)(token_blocks, places)
    by_expert = buffers.reshape(blocks, EXPERTS, CAP, D).transpose(1, 0, 2, 3).reshape(EXPERTS, blocks * CAP, D)
    outputs = lax.map(expert_ffn, (by_expert, w_gate, w_up, w_down))
    home = outputs.reshape(EXPERTS, blocks, CAP, D).transpose(1, 0, 2, 3).reshape(blocks, EXPERTS * CAP, D)
    mixed = jax.vmap(combine_block)(gate_blocks, places, home)
    return mixed.reshape(blocks * TOK_DEV, D)
```

```python
import functools

import jax
import jax.numpy as jnp
from jax import lax
from jax.experimental import pallas as pl
from jax.experimental.pallas import tpu as pltpu
from jax.sharding import PartitionSpec as P

EXPERTS = 8
TOPK = 2
CAP = 3
LANES = 128
SUB = 512
SLOTS = 6
ORDER = (1, 3, 2)


def route_places(ids):
    flat = ids.reshape(-1)
    onehot = (flat[:, None] == jnp.arange(EXPERTS, dtype=jnp.int32)[None, :]).astype(jnp.int32)
    before = jnp.cumsum(onehot, axis=0) - onehot
    slot = jnp.sum(before * onehot, axis=1)
    return flat * CAP + slot


def plain_body(tokens, expert_ids, gates, w_gate, w_up, w_down):
    n_groups = lax.axis_size("expert")
    local_experts = w_gate.shape[0]
    width = tokens.shape[1]
    tok_count = tokens.shape[0]
    places = route_places(expert_ids)
    picker = (jnp.arange(EXPERTS * CAP, dtype=jnp.int32)[:, None] == places[None, :]).astype(
        jnp.bfloat16
    )
    doubled = jnp.repeat(tokens, TOPK, axis=0)
    buffer = jnp.dot(picker, doubled, preferred_element_type=jnp.float32).astype(jnp.bfloat16)
    buffer = buffer.reshape(n_groups, local_experts * CAP, width)
    arrived = lax.all_to_all(buffer, "expert", split_axis=0, concat_axis=0, tiled=True)
    regrouped = arrived.reshape(n_groups, local_experts, CAP, width).transpose(1, 0, 2, 3)
    regrouped = regrouped.reshape(local_experts, n_groups * CAP, width)
    piece = lax.all_gather(regrouped, "tensor", axis=1, tiled=True)
    gate_act = jnp.einsum("erd,edf->erf", piece, w_gate, preferred_element_type=jnp.float32)
    up_act = jnp.einsum("erd,edf->erf", piece, w_up, preferred_element_type=jnp.float32)
    hidden = (jax.nn.silu(gate_act) * up_act).astype(jnp.bfloat16)
    term = jnp.einsum("erf,efd->red", hidden, w_down, preferred_element_type=jnp.float32)
    summed = lax.psum_scatter(
        term.reshape(n_groups * CAP * lax.axis_size("tensor"), local_experts * width).astype(
            jnp.bfloat16
        ),
        "tensor",
        scatter_dimension=0,
        tiled=True,
    )
    results = summed.reshape(n_groups, CAP, local_experts, width)
    returned = lax.all_to_all(results, "expert", split_axis=0, concat_axis=0, tiled=True)
    results_flat = returned.transpose(0, 2, 1, 3).reshape(EXPERTS * CAP, width)
    weights = (jnp.arange(EXPERTS * CAP, dtype=jnp.int32)[None, :] == places[:, None]).astype(
        jnp.float32
    )
    weights = weights * gates.reshape(-1)[:, None]
    weights = jnp.sum(weights.reshape(tok_count, TOPK, EXPERTS * CAP), axis=1)
    mixed = jnp.dot(weights, results_flat.astype(jnp.float32), precision=lax.Precision.HIGHEST)
    return mixed.astype(jnp.bfloat16)


def kernel(
    dims,
    tok, wg, wu, wd, out,
    raw, xs, route, gbuf, ubuf, dbuf, gacc, uacc, hid,
    own, p1, s1, t3, ra, rb, t1, t2, rx, ry, t0, rz,
    gsem, usem, dsem,
    zs, zr, xsend, xrecv, ysend, yrecv, das, dar, dbs, dbr, ss, sr,
    r1s, r1r, r2s, r2r, r3s, r3r, r4s, r4r,
):
    n_exp, width, kc, n_k, nz, rows8 = dims
    f32, bf16 = jnp.float32, jnp.bfloat16
    wide = tok.shape[1]
    cut = (width // 2 // LANES) * LANES
    n_steps = n_exp * n_k
    n_sub = width // SUB
    n_chunk = n_sub // 2
    quarter = nz * rows8
    half = 4 * quarter

    y = lax.axis_index("expert")
    t = lax.axis_index("tensor")
    z, x, c = t // 4, (t // 2) % 2, t % 2

    def at(yy, zz, xx, cc):
        return (yy, (zz * 2 + xx) * 2 + cc)

    xn = at(y, z, 1 - x, c)
    yn = at(1 - y, z, x, c)
    sib = at(y, z, x, 1 - c)
    zn = [at(y, (z + k) % nz, x, c) for k in range(nz)]

    def load_g(s, slot):
        rows = pl.ds(pl.multiple_of((s % n_k) * kc, kc), kc)
        e = s // n_k
        return (
            pltpu.make_async_copy(wg.at[e, rows, :], gbuf.at[slot], gsem.at[slot]),
            pltpu.make_async_copy(wu.at[e, rows, :], ubuf.at[slot], usem.at[slot]),
        )

    def load_d(n):
        cols = pl.ds(pl.multiple_of(n * SUB, SUB), SUB)
        return pltpu.make_async_copy(wd.at[:, :, cols], dbuf.at[n], dsem.at[n])

    for s in range(SLOTS):
        for copy in load_g(s, s):
            copy.start()
    for n in range(n_sub):
        load_d(n).start()

    barrier = pltpu.get_barrier_semaphore()
    peers = [xn, yn, sib] + zn[1:]
    for peer in peers:
        pl.semaphore_signal(barrier, inc=1, device_id=peer, device_id_type=pl.DeviceIdType.MESH)
    pl.semaphore_wait(barrier, len(peers))

    sent = []

    def send(src, dst, ssem, rsem, dev):
        copy = pltpu.make_async_remote_copy(
            src_ref=src, dst_ref=dst, send_sem=ssem, recv_sem=rsem,
            device_id=dev, device_id_type=pl.DeviceIdType.MESH,
        )
        copy.start()
        sent.append(copy)
        return copy

    def mine(j):
        return tok if j == 0 else raw.at[0, 0, j]

    def to_sib(g, j):
        src = mine(j) if g == 0 else raw.at[0, g, j]
        return send(src, raw.at[1, g, j], ss.at[g, j], sr.at[g, j], sib)

    zc, xc, yc, sc, ac, bc = {}, {}, {}, {}, {}, {}
    for k in ORDER:
        j = (nz - k) % nz
        zc[j] = send(tok, raw.at[0, 0, j], zs.at[k], zr.at[j], zn[k])

    def spread(j):
        xc[j] = send(mine(j), raw.at[0, 1, j], xsend.at[j], xrecv.at[j], xn)
        yc[j] = send(mine(j), raw.at[0, 2, j], ysend.at[j], yrecv.at[j], yn)
        sc[0, j] = to_sib(0, j)

    spread(0)
    raw[0, 0, 0] = tok[...]
    for j in ORDER:
        zc[j].wait_recv()
        spread(j)
    for j in (0,) + ORDER:
        xc[j].wait_recv()
        ac[j] = send(
            raw.at[0, 1, j, :, pl.ds(0, cut)], raw.at[0, 3, j, :, pl.ds(0, cut)],
            das.at[j], dar.at[j], yn,
        )
        sc[1, j] = to_sib(1, j)
        yc[j].wait_recv()
        bc[j] = send(
            raw.at[0, 2, j, :, pl.ds(cut, wide - cut)], raw.at[0, 3, j, :, pl.ds(cut, wide - cut)],
            dbs.at[j], dbr.at[j], xn,
        )
        sc[2, j] = to_sib(2, j)

    def settle(a, g):
        r0 = (a * 4 + g) * quarter

        def part(i, _):
            cols = pl.ds(pl.multiple_of(i * SUB, SUB), SUB)
            v = raw[a, g, :, :, cols].astype(f32).reshape(quarter, SUB)
            xs[r0:r0 + quarter, cols] = v.astype(bf16)
            return 0

        lax.fori_loop(0, width // SUB, part, 0)
        v = raw[a, g, :, :, width:wide].astype(f32)
        route[r0:r0 + quarter, :] = v.reshape(quarter, wide - width)

    for g in range(3):
        settle(0, g)
    for g in range(3):
        for j in range(nz):
            sc[g, j].wait_recv()
        settle(1, g)
    for j in (0,) + ORDER:
        ac[j].wait_recv()
        bc[j].wait_recv()
        sc[3, j] = to_sib(3, j)
    settle(0, 3)
    for j in range(nz):
        sc[3, j].wait_recv()
    settle(1, 3)

    def step(s, _):
        slot = s % SLOTS
        for copy in load_g(s, slot):
            copy.wait()
        k = s % n_k
        e = s // n_k
        left = xs[:, pl.ds(pl.multiple_of(k * kc, kc), kc)]
        g = jnp.dot(left, gbuf[slot], preferred_element_type=f32)
        u = jnp.dot(left, ubuf[slot], preferred_element_type=f32)

        @pl.when(k == 0)
        def _():
            gacc[...] = g
            uacc[...] = u

        @pl.when(k > 0)
        def _():
            gacc[...] += g
            uacc[...] += u

        @pl.when(s + SLOTS < n_steps)
        def _():
            for copy in load_g(s + SLOTS, slot):
                copy.start()

        @pl.when(k == n_k - 1)
        def _():
            lane = lax.broadcasted_iota(jnp.int32, route.shape, 1)
            which = y * n_exp + e
            hit = (lane == which) | (lane == which + EXPERTS)
            w = jnp.sum(jnp.where(hit, route[...], 0.0), axis=1, keepdims=True)
            gv = gacc[...]
            hid[e] = (gv / (1.0 + jnp.exp(-gv)) * uacc[...] * w).astype(bf16)

        return 0

    lax.fori_loop(0, n_steps, step, 0)

    def down(n, _):
        load_d(n).wait()
        acc = jnp.dot(hid[0], dbuf[n, 0], preferred_element_type=f32)
        for e in range(1, n_exp):
            acc += jnp.dot(hid[e], dbuf[n, e], preferred_element_type=f32)
        own[n] = acc[:half]
        p1[n] = acc[half:].astype(bf16)
        return 0

    c1, c2, c3, c4 = {}, {}, {}, {}
    q = quarter

    def stage1(i):
        lax.fori_loop(2 * i, 2 * i + 2, down, 0)
        two = pl.ds(2 * i, 2)
        c1[i] = send(p1.at[two], s1.at[two], r1s.at[i], r1r.at[i], sib)

    def stage2(i):
        a, b = 2 * i, 2 * i + 1
        c1[i].wait_recv()
        for n in (a, b):
            t3[n] = (own[n, 3 * q:4 * q] + s1[n, 3 * q:4 * q].astype(f32)).astype(bf16)
        c2[i] = (
            send(t3.at[a], ra.at[i], r2s.at[i, 0], r2r.at[i, 0], yn),
            send(t3.at[b], rb.at[i], r2s.at[i, 1], r2r.at[i, 1], xn),
        )
        for n in (a, b):
            own[n, 0:3 * q] += s1[n, 0:3 * q].astype(f32)

    def stage3(i):
        a, b = 2 * i, 2 * i + 1
        for copy in c2[i]:
            copy.wait_recv()
        t1[a] = (own[a, q:2 * q] + ra[i].astype(f32)).astype(bf16)
        t1[b] = own[b, q:2 * q].astype(bf16)
        t2[a] = own[a, 2 * q:3 * q].astype(bf16)
        t2[b] = (own[b, 2 * q:3 * q] + rb[i].astype(f32)).astype(bf16)
        two = pl.ds(a, 2)
        c3[i] = (
            send(t1.at[two], rx.at[two], r3s.at[i, 0], r3r.at[i, 0], xn),
            send(t2.at[two], ry.at[two], r3s.at[i, 1], r3r.at[i, 1], yn),
        )

    def stage4(i):
        for copy in c3[i]:
            copy.wait_recv()
        for n in (2 * i, 2 * i + 1):
            v = own[n, 0:q] + rx[n].astype(f32) + ry[n].astype(f32)
            own[n, 0:q] = v
            v = v.reshape(nz, rows8, SUB).astype(bf16)
            for k in range(1, nz):
                t0[k, n] = v[k]
        two = pl.ds(2 * i, 2)
        c4[i] = [
            send(t0.at[k, two], rz.at[k, two], r4s.at[i, k], r4r.at[i, k], zn[k])
            for k in range(1, nz)
        ]

    def stage5(i):
        for copy in c4[i]:
            copy.wait_recv()
        for n in (2 * i, 2 * i + 1):
            v = own[n, 0:rows8]
            for k in range(1, nz):
                v += rz[k, n].astype(f32)
            out[:, n * SUB:(n + 1) * SUB] = v.astype(out.dtype)

    stages = (stage1, stage2, stage3, stage4, stage5)
    for tick in range(n_chunk + len(stages) - 1):
        for lag, stage in enumerate(stages):
            if 0 <= tick - lag < n_chunk:
                stage(tick - lag)
    for copy in sent:
        copy.wait_send()


def fused_body(tokens, expert_ids, gates, w_gate, w_up, w_down):
    rows8, width = tokens.shape
    n_exp, _, ff = w_gate.shape
    n_tensor = lax.axis_size("tensor")
    nz = n_tensor // 4
    n_k = 4
    kc = width // n_k
    bf16, f32 = jnp.bfloat16, jnp.float32
    lanes = jnp.arange(EXPERTS, dtype=jnp.int32)
    full = jnp.sum(
        jnp.where(expert_ids[:, :, None] == lanes[None, None, :], gates[:, :, None], 0.0), axis=1
    )
    top = full.astype(bf16)
    low = (full - top.astype(f32)).astype(bf16)
    pad = jnp.zeros((rows8, LANES - 2 * EXPERTS), bf16)
    tok = jnp.concatenate([tokens, top, low, pad], axis=1)
    wide = width + LANES
    rows = 8 * nz * rows8
    q = nz * rows8
    n_sub = width // SUB
    n_chunk = n_sub // 2
    dma = pltpu.SemaphoreType.DMA
    vm = pltpu.VMEM
    scratch = [
        vm((2, 4, nz, rows8, wide), bf16),
        vm((rows, width), bf16),
        vm((rows, LANES), f32),
        vm((SLOTS, kc, ff), bf16),
        vm((SLOTS, kc, ff), bf16),
        vm((n_sub, n_exp, ff, SUB), bf16),
        vm((rows, ff), f32),
        vm((rows, ff), f32),
        vm((n_exp, rows, ff), bf16),
        vm((n_sub, 4 * q, SUB), f32),
        vm((n_sub, 4 * q, SUB), bf16),
        vm((n_sub, 4 * q, SUB), bf16),
        vm((n_sub, q, SUB), bf16),
        vm((n_chunk, q, SUB), bf16),
        vm((n_chunk, q, SUB), bf16),
        vm((n_sub, q, SUB), bf16),
        vm((n_sub, q, SUB), bf16),
        vm((n_sub, q, SUB), bf16),
        vm((n_sub, q, SUB), bf16),
        vm((nz, n_sub, rows8, SUB), bf16),
        vm((nz, n_sub, rows8, SUB), bf16),
        dma((SLOTS,)), dma((SLOTS,)), dma((n_sub,)),
        dma((nz,)), dma((nz,)), dma((nz,)), dma((nz,)), dma((nz,)), dma((nz,)),
        dma((nz,)), dma((nz,)), dma((nz,)), dma((nz,)), dma((4, nz)), dma((4, nz)),
        dma((n_chunk,)), dma((n_chunk,)), dma((n_chunk, 2)), dma((n_chunk, 2)),
        dma((n_chunk, 2)), dma((n_chunk, 2)), dma((n_chunk, nz)), dma((n_chunk, nz)),
    ]
    return pl.pallas_call(
        functools.partial(kernel, (n_exp, width, kc, n_k, nz, rows8)),
        out_shape=jax.ShapeDtypeStruct((rows8, width), bf16),
        in_specs=[pl.BlockSpec(memory_space=pltpu.VMEM)]
        + [pl.BlockSpec(memory_space=pl.ANY)] * 3,
        out_specs=pl.BlockSpec(memory_space=pltpu.VMEM),
        scratch_shapes=scratch,
        compiler_params=pltpu.CompilerParams(
            collective_id=0, has_side_effects=True, vmem_limit_bytes=67043328
        ),
    )(tok, w_gate, w_up, w_down)


def body(tokens, expert_ids, gates, w_gate, w_up, w_down):
    fits = (
        lax.axis_size("expert") == 2
        and lax.axis_size("tensor") == 16
        and tokens.shape[0] == 8
        and w_gate.size * 2 <= 32 * 1024 * 1024
        and w_gate.shape[2] == SUB
        and tokens.shape[1] % (2 * SUB) == 0
    )
    run = fused_body if fits else plain_body
    return run(tokens, expert_ids, gates, w_gate, w_up, w_down)


def solution(mesh):
    return jax.shard_map(
        body,
        mesh=mesh,
        in_specs=(
            P(("expert", "tensor"), None),
            P(("expert", "tensor"), None),
            P(("expert", "tensor"), None),
            P("expert", None, "tensor"),
            P("expert", None, "tensor"),
            P("expert", "tensor", None),
        ),
        out_specs=P(("expert", "tensor"), None),
        check_vma=False,
    )
```
